32 devices in a mesh: gx: 8 (over z, x), gy: 4 (over y, core).
Axes of the slice: x: 2, y: 2, z: 4, core: 2. Of those that a mesh axis runs over, the one named last changes fastest.
Arguments:
- species: float32 [53, 32, 32, 128], P(None, 'gx', 'gy'), may hold values from -6 to 6
- diffusion: float32 [53], replicated, may hold values from 0.02 to 0.15
- class_rate: float32 [4], replicated, may hold values from 0.2 to 1
- mixing: float32 [53, 53], replicated, may hold values from -0.3 to 0.3
- inverses: float32 [4, 53, 53], replicated, may hold values from -0.01 to 0.12
- newton_counts: int32 [4], replicated, may hold values from 1 to 8, as said below
- cell_class: int32 [32, 32, 128], P('gx', 'gy'), may hold values from 0 to 3
Outputs:
- updated: float32 [53, 32, 32, 128], P(None, 'gx', 'gy')
The draws below stay inside these ranges and needn't reach their ends.
Inputs may be any that keep to these rules, and one draw needn't show every extreme that they name: `newton_counts`: nondecreasing in the class; the last class takes 8.
All inputs are finite; a program needn't handle non-finite values.
Results may differ from the reference program's by a relative error of at most 0.0003.
Values sent between devices are 32-bit elements; how exact they have to be, the bound alone decides.
A program may use at most 64 MiB of HBM per device.

```python
import math
import jax
import jax.numpy as jnp
from jax import lax

SPEC = 53
NCLASS = 4
NMAX = 8
NZ = 128
NX = 32
NY = 32


def draw_inverses(key, part):
    first, second = jax.random.split(jax.random.fold_in(key, 5))
    diag = jnp.exp(jax.random.uniform(first, (NCLASS, SPEC), jnp.float32, math.log(0.06), math.log(0.12)))
    spread = jax.random.normal(second, (NCLASS, SPEC, SPEC), jnp.float32)
    spread = jnp.clip(spread * (0.0225 / math.sqrt(SPEC)), -0.01, 0.01)
    identity = jnp.eye(SPEC, dtype=jnp.float32)[None]
    return spread * (1.0 - identity) + diag[:, :, None] * identity


def draw_newton_counts(key, part):
    base = jax.random.randint(jax.random.fold_in(key, 11), (NCLASS,), 1, NMAX + 1)
    base = jnp.sort(base)
    return base.at[NCLASS - 1].set(NMAX).astype(jnp.int32)


def draw_cell_class(key, part):
    front_key, heavy_key, pick_key, light_key = jax.random.split(jax.random.fold_in(key, 23), 4)
    front = jax.random.randint(front_key, (), 0, NX)
    positions = jnp.arange(NX, dtype=jnp.int32)[:, None, None]
    near = jnp.abs(positions - front) < max(NX // 16, 1)
    shape = (NX, NY, NZ)
    heavy = jax.random.randint(heavy_key, shape, 1, NCLASS)
    picked = jax.random.randint(pick_key, shape, 0, 8)
    light = jnp.where(picked == 0, jax.random.randint(light_key, shape, 0, NCLASS), 0)
    return jnp.where(near, heavy, light).astype(jnp.int32)


def level_of(stream_key, shape, shards, least, largest):
    gain = 1.0
    for dim, shards_of in shards:
        draws = jax.random.uniform(jax.random.fold_in(jax.random.fold_in(stream_key, 6), dim), (shards_of,), jnp.float32, least / len(shards), largest / len(shards))
        gain = gain * jnp.repeat(jnp.exp(draws), shape[dim] // shards_of).reshape((-1,) + (1,) * (len(shape) - 1 - dim))
    return gain


def normal_values(own_key, extent, scale, bound, cuts=(), held_as=jnp.bfloat16):
    level = level_of(own_key, extent, cuts, -0.22, 0.18) if cuts else 1.0
    values = jax.random.normal(own_key, extent, jnp.float32) * scale * level
    return jnp.minimum(jnp.maximum(values, -bound), bound).astype(held_as)


def setup_inputs(seed: int = 0) -> dict:
    arg_keys = jax.random.split(jax.random.key(seed), 8)
    species = normal_values(arg_keys[0], (SPEC, NX, NY, NZ), 1.0, 6.0, ((1, 8), (2, 4)), jnp.float32)
    diffusion = jnp.clip(jnp.exp(jax.random.uniform(arg_keys[1], (SPEC,), jnp.float32, math.log(0.02), math.log(0.15))), 0.02, 0.15)
    class_rate = jnp.clip(jnp.exp(jax.random.uniform(arg_keys[2], (NCLASS,), jnp.float32, math.log(0.2), math.log(1.0))), 0.2, 1.0)
    mixing = normal_values(arg_keys[3], (SPEC, SPEC), (0.3 * SPEC ** -0.5), 0.3, (), jnp.float32)
    inverses = draw_inverses(jax.random.fold_in(arg_keys[7], 71), 0)
    newton_counts = draw_newton_counts(jax.random.fold_in(arg_keys[7], 71), 0)
    cell_class = draw_cell_class(jax.random.fold_in(arg_keys[7], 71), 0)
    return {"species": species, "diffusion": diffusion, "class_rate": class_rate, "mixing": mixing, "inverses": inverses, "newton_counts": newton_counts, "cell_class": cell_class}


def laplace(grid_field):
    padded = jnp.pad(grid_field, 1)
    total = padded[2:, 1:-1, 1:-1] + padded[:-2, 1:-1, 1:-1]
    total = total + padded[1:-1, 2:, 1:-1] + padded[1:-1, :-2, 1:-1]
    total = total + padded[1:-1, 1:-1, 2:] + padded[1:-1, 1:-1, :-2]
    return total - 6.0 * grid_field


def newton_cells(target, classes, class_rate, mixing, inverses, newton_counts):
    class_mask = (classes[None, :] == jnp.arange(NCLASS, dtype=jnp.int32)[:, None])
    weights = class_mask.astype(jnp.float32)
    cell_rate = jnp.sum(class_rate[:, None] * weights, axis=0)
    cell_count = jnp.sum(jnp.where(class_mask, newton_counts[:, None], 0), axis=0)

    def newton_step(k, state):
        source = jnp.dot(mixing, jnp.tanh(state), precision=lax.Precision.HIGHEST) - state
        residual = state - target - cell_rate * source
        correction = jnp.zeros_like(state)
        for which in range(NCLASS):
            correction = correction + weights[which] * jnp.dot(inverses[which], residual, precision=lax.Precision.HIGHEST)
        return jnp.where(k < cell_count, state - correction, state)

    return lax.fori_loop(0, NMAX, newton_step, target)


def reference(species, diffusion, class_rate, mixing, inverses, newton_counts, cell_class):
    forcing = lax.map(laplace, species) * diffusion[:, None, None, None]
    target = species + forcing
    moved = jnp.moveaxis(target, 1, 0)

    def solve_slice(pair):
        slab, slab_class = pair
        solved = newton_cells(slab.reshape(SPEC, -1), slab_class.reshape(-1), class_rate, mixing, inverses, newton_counts)
        return solved.reshape(slab.shape)

    section_value = jnp.moveaxis(lax.map(solve_slice, (moved, cell_class)), 0, 1)
    second = lax.map(laplace, section_value) * diffusion[:, None, None, None]
    return section_value + 0.5 * (second - forcing)
```

```python
import functools

import jax
import jax.numpy as jnp
from jax import lax
from jax.experimental import pallas as pl
from jax.experimental.pallas import tpu as pltpu
from jax.sharding import PartitionSpec as P

NMAX = 8
CHUNK = 2
MESH = pl.DeviceIdType.MESH
F32 = jnp.float32
BF16 = jnp.bfloat16


def kernel(
    dims,
    species_hbm, diffusion_ref, rate_ref, mixing_ref, inverses_ref, counts_ref, class_ref,
    out_ref,
    raw, ext, ext2, forcing, target, coef, square, mix_w, inv_w,
    load_sem, xs_send, xs_recv, ys_send, ys_recv,
):
    spec, nx, ny, nz, nclass = dims
    rows = nx * ny
    pad = ext.shape[2]
    chunks = ny // CHUNK
    gx, gy = lax.axis_index("gx"), lax.axis_index("gy")
    sx, sy = lax.axis_size("gx"), lax.axis_size("gy")
    has_x = (gx > 0, gx < sx - 1)
    has_y = (gy > 0, gy < sy - 1)
    to_x = ((gx - 1, gy), (gx + 1, gy))
    to_y = ((gx, gy - 1), (gx, gy + 1))

    load = pltpu.make_async_copy(species_hbm, raw, load_sem)
    load.start()

    barrier = pltpu.get_barrier_semaphore()
    for has, to in zip(has_x + has_y, to_x + to_y):
        @pl.when(has)
        def _():
            pl.semaphore_signal(barrier, inc=1, device_id=to, device_id_type=MESH)

    def x_copy(stage, side, c):
        buf = (ext, ext2)[stage]
        src_row, dst_row = (1, nx + 1) if side == 0 else (nx, 0)
        ys = pl.ds(1 + c * CHUNK, CHUNK)
        return pltpu.make_async_remote_copy(
            src_ref=buf.at[src_row, ys], dst_ref=buf.at[dst_row, ys],
            send_sem=xs_send.at[stage, side, c], recv_sem=xs_recv.at[stage, side, c],
            device_id=to_x[side], device_id_type=MESH)

    def y_copy(stage, side):
        buf = (ext, ext2)[stage]
        src_col, dst_col = (1, ny + 1) if side == 0 else (ny, 0)
        return pltpu.make_async_remote_copy(
            src_ref=buf.at[pl.ds(1, nx), src_col], dst_ref=buf.at[pl.ds(1, nx), dst_col],
            send_sem=ys_send.at[stage, side], recv_sem=ys_recv.at[stage, side],
            device_id=to_y[side], device_id_type=MESH)

    def x_arrive(stage, c):
        for side in (0, 1):
            @pl.when(has_x[side])
            def _():
                x_copy(stage, 1 - side, c).wait_recv()

    def y_arrive(stage):
        for side in (0, 1):
            @pl.when(has_y[side])
            def _():
                y_copy(stage, 1 - side).wait_recv()

    zero_col = jnp.zeros((pad, nz), F32)
    for side in (0, 1):
        @pl.when(jnp.logical_not(has_x[side]))
        def _():
            for buf in (ext, ext2):
                for y in range(ny):
                    buf[(0, nx + 1)[side], y + 1] = zero_col
        @pl.when(jnp.logical_not(has_y[side]))
        def _():
            for buf in (ext, ext2):
                for x in range(nx):
                    buf[x + 1, (0, ny + 1)[side]] = zero_col

    load.wait()

    def relay(x):
        for y in range(ny):
            col = raw[pl.ds(x * ny + y, spec, stride=rows), :]
            ext[x + 1, y + 1] = jnp.concatenate([col, jnp.zeros((pad - spec, nz), F32)], axis=0)

    relay(0)
    relay(nx - 1)
    neighbours = sum(has.astype(jnp.int32) for has in has_x + has_y)
    pl.semaphore_wait(barrier, neighbours)
    for c in range(chunks):
        for side in (0, 1):
            @pl.when(has_x[side])
            def _():
                x_copy(0, side, c).start()
    for x in range(1, nx - 1):
        relay(x)
    for side in (0, 1):
        @pl.when(has_y[side])
        def _():
            y_copy(0, side).start()

    square[...] = jnp.zeros_like(square)

    def split_weight(value):
        square[0:spec, 0:spec] = value
        w = square[...]
        high = w.astype(BF16).astype(F32)
        both = (high + pltpu.roll(w - high, 64, 1)).astype(BF16)
        return jnp.concatenate([both, both], axis=1)

    mix_w[...] = split_weight(mixing_ref[...])
    for k in range(nclass):
        inv_w[k * 64:(k + 1) * 64, :] = split_weight(inverses_ref[k])
    square[...] = jnp.zeros_like(square)
    square[0:1, 0:spec] = diffusion_ref[...]
    line = jnp.broadcast_to(square[0:1, :], square.shape)
    on = lax.broadcasted_iota(jnp.int32, square.shape, 0) == lax.broadcasted_iota(
        jnp.int32, square.shape, 1)
    column = jnp.sum(jnp.where(on, line, 0.0), axis=1, keepdims=True)
    coef[...] = jnp.broadcast_to(column[:pad], coef.shape)

    lane = lax.broadcasted_iota(jnp.int32, (pad, nz), 1)

    def laplace(buf, x, y):
        v = buf[x + 1, y + 1]
        total = buf[x + 2, y + 1] + buf[x, y + 1] + buf[x + 1, y + 2] + buf[x + 1, y]
        total = total + jnp.where(lane == nz - 1, 0.0, pltpu.roll(v, nz - 1, 1))
        total = total + jnp.where(lane == 0, 0.0, pltpu.roll(v, 1, 1))
        return v, total - 6.0 * v

    def split_rows(v):
        v = jnp.concatenate([v, jnp.zeros((64 - pad, v.shape[1]), F32)], axis=0)
        high = v.astype(BF16)
        low = (v - high.astype(F32)).astype(BF16)
        return jnp.concatenate([high, high, low, low], axis=0)

    def solve(xs, c):
        cells = [(x, c * CHUNK + j) for x in xs for j in range(CHUNK)]
        parts = []
        for x, y in cells:
            v, lap = laplace(ext, x, y)
            force = coef[...] * lap
            forcing[x, y] = force
            parts.append(v + force)
        start = jnp.concatenate(parts, axis=1)
        target[...] = start
        which = jnp.concatenate([class_ref[pl.ds(x * ny + y, 1), :] for x, y in cells], axis=1)
        cell_rate = jnp.zeros(which.shape, F32)
        cell_count = jnp.zeros(which.shape, jnp.int32)
        for k in range(nclass):
            cell_rate = jnp.where(which == k, rate_ref[k], cell_rate)
            cell_count = jnp.where(which == k, counts_ref[k], cell_count)

        def step(k, y):
            product = jnp.dot(mix_w[...], split_rows(jnp.tanh(y)), preferred_element_type=F32)[:pad]
            residual = y - target[...] - cell_rate * (product - y)
            fixes = jnp.dot(inv_w[...], split_rows(residual), preferred_element_type=F32)
            active = jnp.where(k < cell_count, which, nclass)
            fix = jnp.zeros_like(y)
            for n in range(nclass):
                fix = jnp.where(active == n, fixes[n * 64:n * 64 + pad], fix)
            return y - fix

        value = lax.fori_loop(0, NMAX, step, start)
        for i, (x, y) in enumerate(cells):
            ext2[x + 1, y + 1] = value[:, i * nz:(i + 1) * nz]

    y_arrive(0)

    def inner(c, carry):
        solve(tuple(range(1, nx - 1)), c)
        return carry

    def outer(c, carry):
        x_arrive(0, c)
        solve((0, nx - 1), c)
        for side in (0, 1):
            @pl.when(has_x[side])
            def _():
                x_copy(1, side, c).start()
        return carry

    if nx > 2:
        lax.fori_loop(0, chunks, inner, 0)
    lax.fori_loop(0, chunks, outer, 0)
    for side in (0, 1):
        @pl.when(has_y[side])
        def _():
            y_copy(1, side).start()

    def finish(x, y):
        v, lap = laplace(ext2, x, y)
        new = v + 0.5 * (coef[...] * lap - forcing[x, y])
        out_ref[pl.ds(x * ny + y, spec, stride=rows), :] = new[:spec]

    for x in range(1, nx - 1):
        for y in range(1, ny - 1):
            finish(x, y)
    y_arrive(1)
    for x in range(1, nx - 1):
        finish(x, 0)
        finish(x, ny - 1)

    def last(c, carry):
        x_arrive(1, c)
        for j in range(CHUNK):
            for x in (0, nx - 1):
                finish(x, c * CHUNK + j)
        return carry

    lax.fori_loop(0, chunks, last, 0)

    for stage in (0, 1):
        for side in (0, 1):
            @pl.when(has_x[side])
            def _():
                for c in range(chunks):
                    x_copy(stage, side, c).wait_send()
            @pl.when(has_y[side])
            def _():
                y_copy(stage, side).wait_send()


def local(species, diffusion, class_rate, mixing, inverses, newton_counts, cell_class):
    spec, nx, ny, nz = species.shape
    nclass = inverses.shape[0]
    pad = -(-spec // 8) * 8
    chunks = ny // CHUNK
    width = 2 * CHUNK * nz
    vmem = pl.BlockSpec(memory_space=pltpu.VMEM)
    smem = pl.BlockSpec(memory_space=pltpu.SMEM)
    out = pl.pallas_call(
        functools.partial(kernel, (spec, nx, ny, nz, nclass)),
        out_shape=jax.ShapeDtypeStruct((spec * nx * ny, nz), F32),
        in_specs=[pl.BlockSpec(memory_space=pl.ANY), vmem, smem, vmem, vmem, smem, vmem],
        out_specs=vmem,
        scratch_shapes=[
            pltpu.VMEM((spec * nx * ny, nz), F32),
            pltpu.VMEM((nx + 2, ny + 2, pad, nz), F32),
            pltpu.VMEM((nx + 2, ny + 2, pad, nz), F32),
            pltpu.VMEM((nx, ny, pad, nz), F32),
            pltpu.VMEM((pad, width), F32),
            pltpu.VMEM((pad, nz), F32),
            pltpu.VMEM((64, 128), F32),
            pltpu.VMEM((64, 256), BF16),
            pltpu.VMEM((nclass * 64, 256), BF16),
            pltpu.SemaphoreType.DMA(()),
            pltpu.SemaphoreType.DMA((2, 2, chunks)),
            pltpu.SemaphoreType.DMA((2, 2, chunks)),
            pltpu.SemaphoreType.DMA((2, 2)),
            pltpu.SemaphoreType.DMA((2, 2)),
        ],
        compiler_params=pltpu.CompilerParams(
            collective_id=0, has_side_effects=True, vmem_limit_bytes=40 * 1024 * 1024),
    )(
        species.reshape(spec * nx * ny, nz), diffusion.reshape(1, spec), class_rate,
        mixing, inverses, newton_counts, cell_class.reshape(nx * ny, nz),
    )
    return out.reshape(species.shape)


def solution(mesh):
    in_specs = (P(None, "gx", "gy", None), P(), P(), P(), P(), P(), P("gx", "gy", None))
    out_specs = P(None, "gx", "gy", None)
    return jax.shard_map(local, mesh=mesh, in_specs=in_specs, out_specs=out_specs, check_vma=False)
```

```python
import functools

import jax
import jax.numpy as jnp
from jax import lax
from jax.experimental import pallas as pl
from jax.experimental.pallas import tpu as pltpu
from jax.sharding import PartitionSpec as P

NMAX = 8
CHUNK = 2
GROUP = 1
SPAN = 4
UNROLL = 4
MESH = pl.DeviceIdType.MESH
F32 = jnp.float32
BF16 = jnp.bfloat16


def kernel(
    dims,
    species_hbm, diffusion_ref, rate_ref, mixing_ref, inverses_ref, counts_ref, class_ref,
    out_ref,
    raw, ext, ext2, forcing, target, coef, square, mix_w, inv_w,
    load_sem, xs_send, xs_recv, ys_send, ys_recv,
):
    spec, nx, ny, nz, nclass = dims
    rows = nx * ny
    pad = ext.shape[2]
    chunks = ny // CHUNK
    gx, gy = lax.axis_index("gx"), lax.axis_index("gy")
    sx, sy = lax.axis_size("gx"), lax.axis_size("gy")
    has_x = (gx > 0, gx < sx - 1)
    has_y = (gy > 0, gy < sy - 1)
    to_x = ((gx - 1, gy), (gx + 1, gy))
    to_y = ((gx, gy - 1), (gx, gy + 1))

    load = pltpu.make_async_copy(species_hbm, raw, load_sem)
    load.start()

    zero_col = jnp.zeros((pad, nz), F32)
    for buf in (ext, ext2):
        for y in range(ny):
            buf[0, y + 1] = zero_col
            buf[nx + 1, y + 1] = zero_col
        for x in range(nx):
            buf[x + 1, 0] = zero_col
            buf[x + 1, ny + 1] = zero_col

    barrier = pltpu.get_barrier_semaphore()
    for has, to in zip(has_x + has_y, to_x + to_y):
        @pl.when(has)
        def _():
            pl.semaphore_signal(barrier, inc=1, device_id=to, device_id_type=MESH)

    def x_copy(stage, side, c):
        buf = (ext, ext2)[stage]
        src_row, dst_row = (1, nx + 1) if side == 0 else (nx, 0)
        ys = pl.ds(1 + c * CHUNK, CHUNK)
        return pltpu.make_async_remote_copy(
            src_ref=buf.at[src_row, ys, pl.ds(0, spec)], dst_ref=buf.at[dst_row, ys, pl.ds(0, spec)],
            send_sem=xs_send.at[stage, side, c], recv_sem=xs_recv.at[stage, side, c],
            device_id=to_x[side], device_id_type=MESH)

    def y_copy(stage, side):
        buf = (ext, ext2)[stage]
        src_col, dst_col = (1, ny + 1) if side == 0 else (ny, 0)
        return pltpu.make_async_remote_copy(
            src_ref=buf.at[pl.ds(1, nx), src_col, pl.ds(0, spec)],
            dst_ref=buf.at[pl.ds(1, nx), dst_col, pl.ds(0, spec)],
            send_sem=ys_send.at[stage, side], recv_sem=ys_recv.at[stage, side],
            device_id=to_y[side], device_id_type=MESH)

    def x_arrive(stage, c):
        for side in (0, 1):
            @pl.when(has_x[side])
            def _():
                x_copy(stage, 1 - side, c).wait_recv()

    def y_arrive(stage):
        for side in (0, 1):
            @pl.when(has_y[side])
            def _():
                y_copy(stage, 1 - side).wait_recv()

    load.wait()

    def relay(x):
        for y in range(ny):
            col = raw[pl.ds(x * ny + y, spec, stride=rows), :]
            ext[x + 1, y + 1] = jnp.concatenate([col, jnp.zeros((pad - spec, nz), F32)], axis=0)

    relay(0)
    relay(nx - 1)
    neighbours = sum(has.astype(jnp.int32) for has in has_x + has_y)
    pl.semaphore_wait(barrier, neighbours)
    for c in range(chunks):
        for side in (0, 1):
            @pl.when(has_x[side])
            def _():
                x_copy(0, side, c).start()
    for x in range(1, nx - 1):
        relay(x)
    for side in (0, 1):
        @pl.when(has_y[side])
        def _():
            y_copy(0, side).start()

    square[...] = jnp.zeros_like(square)

    def split_weight(value):
        square[0:spec, 0:spec] = value
        w = square[...]
        high = w.astype(BF16).astype(F32)
        both = high + pltpu.roll((w - high).astype(BF16).astype(F32), 64, 1)
        return jnp.concatenate([both, both], axis=1)[:, :192]

    mix_w[...] = split_weight(mixing_ref[...]).astype(BF16)
    inv_w[...] = jnp.concatenate(
        [split_weight(inverses_ref[:, k, :])[:pad] for k in range(nclass)], axis=0).astype(BF16)
    square[...] = jnp.zeros_like(square)
    square[0:1, 0:spec] = diffusion_ref[...]
    line = jnp.broadcast_to(square[0:1, :], square.shape)
    on = lax.broadcasted_iota(jnp.int32, square.shape, 0) == lax.broadcasted_iota(
        jnp.int32, square.shape, 1)
    column = jnp.sum(jnp.where(on, line, 0.0), axis=1, keepdims=True)
    coef[...] = jnp.broadcast_to(column[:pad], coef.shape)

    lane = lax.broadcasted_iota(jnp.int32, (pad, nz), 1)

    def laplace(buf, x, y):
        v = buf[x + 1, y + 1]
        total = buf[x + 2, y + 1] + buf[x, y + 1] + buf[x + 1, y + 2] + buf[x + 1, y]
        total = total + jnp.where(lane == nz - 1, 0.0, pltpu.roll(v, nz - 1, 1))
        total = total + jnp.where(lane == 0, 0.0, pltpu.roll(v, 1, 1))
        return v, total - 6.0 * v

    def split_rows(v):
        v = jnp.concatenate([v, jnp.zeros((64 - pad, v.shape[1]), F32)], axis=0)
        high = v.astype(BF16)
        low = (v - high.astype(F32)).astype(BF16)
        return jnp.concatenate([high, high, low], axis=0)

    def solve(xs, first):
        groups = [[(x, first + g * GROUP + j) for x in xs for j in range(GROUP)]
                  for g in range(SPAN // GROUP)]
        starts, rates, whiches, limits = [], [], [], []
        for g, cells in enumerate(groups):
            parts = []
            for x, y in cells:
                v, lap = laplace(ext, x, y)
                force = coef[...] * lap
                forcing[x, y] = force
                parts.append(v + force)
            start = jnp.concatenate(parts, axis=1)
            target[g] = start
            which = jnp.concatenate([class_ref[pl.ds(x * ny + y, 1), :] for x, y in cells], axis=1)
            cell_rate = jnp.zeros(which.shape, F32)
            cell_count = jnp.zeros(which.shape, jnp.int32)
            for k in range(nclass):
                cell_rate = jnp.where(which == k, rate_ref[k], cell_rate)
                cell_count = jnp.where(which == k, counts_ref[k], cell_count)
            starts.append(start)
            rates.append(cell_rate)
            whiches.append(which)
            limits.append(cell_count)

        def step(k, ys):
            out = []
            for g, y in enumerate(ys):
                product = jnp.dot(mix_w[...], split_rows(jnp.tanh(y)), preferred_element_type=F32)[:pad]
                residual = y - target[g] - rates[g] * (product - y)
                fixes = jnp.dot(inv_w[...], split_rows(residual), preferred_element_type=F32)
                active = jnp.where(k < limits[g], whiches[g], nclass)
                fix = jnp.zeros_like(y)
                for n in range(nclass):
                    fix = jnp.where(active == n, fixes[n * pad:(n + 1) * pad], fix)
                out.append(y - fix)
            return tuple(out)

        values = lax.fori_loop(0, NMAX, step, tuple(starts), unroll=UNROLL)
        for cells, value in zip(groups, values):
            for i, (x, y) in enumerate(cells):
                ext2[x + 1, y + 1] = value[:, i * nz:(i + 1) * nz]

    y_arrive(0)

    def inner(c, carry):
        solve(tuple(range(1, nx - 1)), c * SPAN)
        return carry

    def outer(c, carry):
        per = SPAN // CHUNK
        for i in range(per):
            x_arrive(0, c * per + i)
        solve((0, nx - 1), c * SPAN)
        for side in (0, 1):
            @pl.when(has_x[side])
            def _():
                for i in range(per):
                    x_copy(1, side, c * per + i).start()
        return carry

    spans = ny // SPAN
    early = (spans + 1) // 2
    if nx > 2:
        lax.fori_loop(0, early, inner, 0)
    lax.fori_loop(0, spans, outer, 0)
    if nx > 2:
        lax.fori_loop(early, spans, inner, 0)
    for side in (0, 1):
        @pl.when(has_y[side])
        def _():
            y_copy(1, side).start()

    def finish(x, y):
        v, lap = laplace(ext2, x, y)
        new = v + 0.5 * (coef[...] * lap - forcing[x, y])
        out_ref[pl.ds(x * ny + y, spec, stride=rows), :] = new[:spec]

    for x in range(1, nx - 1):
        for y in range(1, ny - 1):
            finish(x, y)
    y_arrive(1)
    for x in range(1, nx - 1):
        finish(x, 0)
        finish(x, ny - 1)

    def last(c, carry):
        x_arrive(1, c)
        for j in range(CHUNK):
            for x in (0, nx - 1):
                finish(x, c * CHUNK + j)
        return carry

    lax.fori_loop(0, chunks, last, 0)

    for stage in (0, 1):
        for side in (0, 1):
            @pl.when(has_x[side])
            def _():
                for c in range(chunks):
                    x_copy(stage, side, c).wait_send()
            @pl.when(has_y[side])
            def _():
                y_copy(stage, side).wait_send()


def local(species, diffusion, class_rate, mixing, inverses, newton_counts, cell_class):
    spec, nx, ny, nz = species.shape
    nclass = inverses.shape[0]
    pad = -(-spec // 8) * 8
    chunks = ny // CHUNK
    width = 2 * GROUP * nz
    vmem = pl.BlockSpec(memory_space=pltpu.VMEM)
    smem = pl.BlockSpec(memory_space=pltpu.SMEM)
    out = pl.pallas_call(
        functools.partial(kernel, (spec, nx, ny, nz, nclass)),
        out_shape=jax.ShapeDtypeStruct((spec * nx * ny, nz), F32),
        in_specs=[pl.BlockSpec(memory_space=pl.ANY), vmem, smem, vmem, vmem, smem, vmem],
        out_specs=vmem,
        scratch_shapes=[
            pltpu.VMEM((spec * nx * ny, nz), F32),
            pltpu.VMEM((nx + 2, ny + 2, pad, nz), F32),
            pltpu.VMEM((nx + 2, ny + 2, pad, nz), F32),
            pltpu.VMEM((nx, ny, pad, nz), F32),
            pltpu.VMEM((SPAN // GROUP, pad, width), F32),
            pltpu.VMEM((pad, nz), F32),
            pltpu.VMEM((64, 128), F32),
            pltpu.VMEM((64, 192), BF16),
            pltpu.VMEM((nclass * pad, 192), BF16),
            pltpu.SemaphoreType.DMA(()),
            pltpu.SemaphoreType.DMA((2, 2, chunks)),
            pltpu.SemaphoreType.DMA((2, 2, chunks)),
            pltpu.SemaphoreType.DMA((2, 2)),
            pltpu.SemaphoreType.DMA((2, 2)),
        ],
        compiler_params=pltpu.CompilerParams(
            collective_id=0, has_side_effects=True, vmem_limit_bytes=60 * 1024 * 1024),
    )(
        species.reshape(spec * nx * ny, nz), diffusion.reshape(1, spec), class_rate,
        mixing, inverses.transpose(1, 0, 2), newton_counts, cell_class.reshape(nx * ny, nz),
    )
    return out.reshape(species.shape)


def solution(mesh):
    in_specs = (P(None, "gx", "gy", None), P(), P(), P(), P(), P(), P("gx", "gy", None))
    out_specs = P(None, "gx", "gy", None)
    return jax.shard_map(local, mesh=mesh, in_specs=in_specs, out_specs=out_specs, check_vma=False)
```

```python
import functools

import jax
import jax.numpy as jnp
from jax import lax
from jax.experimental import pallas as pl
from jax.experimental.pallas import tpu as pltpu
from jax.sharding import PartitionSpec as P

NMAX = 8
CHUNK = 2
GROUP = 1
SPAN = 4
UNROLL = 8
MESH = pl.DeviceIdType.MESH
F32 = jnp.float32
BF16 = jnp.bfloat16


def kernel(
    dims,
    species_hbm, diffusion_ref, rate_ref, mixing_ref, inverses_ref, counts_ref, class_ref,
    out_ref,
    raw, ext, ext2, forcing, target, coef, square, mix_w, inv_w,
    load_sem, xs_send, xs_recv, ys_send, ys_recv,
):
    spec, nx, ny, nz, nclass = dims
    rows = nx * ny
    pad = ext.shape[2]
    chunks = ny // CHUNK
    gx, gy = lax.axis_index("gx"), lax.axis_index("gy")
    sx, sy = lax.axis_size("gx"), lax.axis_size("gy")
    has_x = (gx > 0, gx < sx - 1)
    has_y = (gy > 0, gy < sy - 1)
    to_x = ((gx - 1, gy), (gx + 1, gy))
    to_y = ((gx, gy - 1), (gx, gy + 1))

    load = pltpu.make_async_copy(species_hbm, raw, load_sem)
    load.start()

    zero_col = jnp.zeros((pad, nz), F32)
    for buf in (ext, ext2):
        for y in range(ny):
            buf[0, y + 1] = zero_col
            buf[nx + 1, y + 1] = zero_col
        for x in range(nx):
            buf[x + 1, 0] = zero_col
            buf[x + 1, ny + 1] = zero_col

    barrier = pltpu.get_barrier_semaphore()
    for has, to in zip(has_x + has_y, to_x + to_y):
        @pl.when(has)
        def _():
            pl.semaphore_signal(barrier, inc=1, device_id=to, device_id_type=MESH)

    def x_copy(stage, side, c):
        buf = (ext, ext2)[stage]
        src_row, dst_row = (1, nx + 1) if side == 0 else (nx, 0)
        ys = pl.ds(1 + c * CHUNK, CHUNK)
        return pltpu.make_async_remote_copy(
            src_ref=buf.at[src_row, ys, pl.ds(0, spec)], dst_ref=buf.at[dst_row, ys, pl.ds(0, spec)],
            send_sem=xs_send.at[stage, side, c], recv_sem=xs_recv.at[stage, side, c],
            device_id=to_x[side], device_id_type=MESH)

    def y_copy(stage, side):
        buf = (ext, ext2)[stage]
        src_col, dst_col = (1, ny + 1) if side == 0 else (ny, 0)
        return pltpu.make_async_remote_copy(
            src_ref=buf.at[pl.ds(1, nx), src_col, pl.ds(0, spec)],
            dst_ref=buf.at[pl.ds(1, nx), dst_col, pl.ds(0, spec)],
            send_sem=ys_send.at[stage, side], recv_sem=ys_recv.at[stage, side],
            device_id=to_y[side], device_id_type=MESH)

    def x_arrive(stage, c):
        for side in (0, 1):
            @pl.when(has_x[side])
            def _():
                x_copy(stage, 1 - side, c).wait_recv()

    def y_arrive(stage):
        for side in (0, 1):
            @pl.when(has_y[side])
            def _():
                y_copy(stage, 1 - side).wait_recv()

    load.wait()

    def relay(x):
        for y in range(ny):
            col = raw[pl.ds(x * ny + y, spec, stride=rows), :]
            ext[x + 1, y + 1] = jnp.concatenate([col, jnp.zeros((pad - spec, nz), F32)], axis=0)

    relay(0)
    relay(nx - 1)
    neighbours = sum(has.astype(jnp.int32) for has in has_x + has_y)
    pl.semaphore_wait(barrier, neighbours)
    for c in range(chunks):
        for side in (0, 1):
            @pl.when(has_x[side])
            def _():
                x_copy(0, side, c).start()
    for x in range(1, nx - 1):
        relay(x)
    for side in (0, 1):
        @pl.when(has_y[side])
        def _():
            y_copy(0, side).start()

    square[...] = jnp.zeros_like(square)

    def split_weight(value):
        square[0:spec, 0:spec] = value
        w = square[...]
        high = w.astype(BF16).astype(F32)
        both = high + pltpu.roll((w - high).astype(BF16).astype(F32), 64, 1)
        return jnp.concatenate([both, both], axis=1)[:, :192]

    mix_w[...] = split_weight(mixing_ref[...]).astype(BF16)
    inv_w[...] = jnp.concatenate(
        [split_weight(inverses_ref[:, k, :])[:pad] for k in range(nclass)], axis=0).astype(BF16)
    square[...] = jnp.zeros_like(square)
    square[0:1, 0:spec] = diffusion_ref[...]
    line = jnp.broadcast_to(square[0:1, :], square.shape)
    on = lax.broadcasted_iota(jnp.int32, square.shape, 0) == lax.broadcasted_iota(
        jnp.int32, square.shape, 1)
    column = jnp.sum(jnp.where(on, line, 0.0), axis=1, keepdims=True)
    coef[...] = jnp.broadcast_to(column[:pad], coef.shape)

    lane = lax.broadcasted_iota(jnp.int32, (pad, nz), 1)

    def laplace(buf, x, y):
        v = buf[x + 1, y + 1]
        total = buf[x + 2, y + 1] + buf[x, y + 1] + buf[x + 1, y + 2] + buf[x + 1, y]
        total = total + jnp.where(lane == nz - 1, 0.0, pltpu.roll(v, nz - 1, 1))
        total = total + jnp.where(lane == 0, 0.0, pltpu.roll(v, 1, 1))
        return v, total - 6.0 * v

    def split_rows(v):
        v = jnp.concatenate([v, jnp.zeros((64 - pad, v.shape[1]), F32)], axis=0)
        high = v.astype(BF16)
        low = (v - high.astype(F32)).astype(BF16)
        return jnp.concatenate([high, high, low], axis=0)

    def solve(xs, first):
        groups = [[(x, first + g * GROUP + j) for x in xs for j in range(GROUP)]
                  for g in range(SPAN // GROUP)]
        starts, rates, whiches, limits = [], [], [], []
        for g, cells in enumerate(groups):
            parts = []
            for x, y in cells:
                v, lap = laplace(ext, x, y)
                force = coef[...] * lap
                forcing[x, y] = force
                parts.append(v + force)
            start = jnp.concatenate(parts, axis=1)
            target[g] = start
            which = jnp.concatenate([class_ref[pl.ds(x * ny + y, 1), :] for x, y in cells], axis=1)
            cell_rate = jnp.zeros(which.shape, F32)
            cell_count = jnp.zeros(which.shape, jnp.int32)
            for k in range(nclass):
                cell_rate = jnp.where(which == k, rate_ref[k], cell_rate)
                cell_count = jnp.where(which == k, counts_ref[k], cell_count)
            starts.append(start)
            rates.append(cell_rate)
            whiches.append(which)
            limits.append(cell_count)

        def step(k, ys):
            out = []
            for g, y in enumerate(ys):
                product = jnp.dot(mix_w[...], split_rows(jnp.tanh(y)), preferred_element_type=F32)[:pad]
                residual = y - target[g] - rates[g] * (product - y)
                fixes = jnp.dot(inv_w[...], split_rows(residual), preferred_element_type=F32)
                active = jnp.where(k < limits[g], whiches[g], nclass)
                fix = jnp.zeros_like(y)
                for n in range(nclass):
                    fix = jnp.where(active == n, fixes[n * pad:(n + 1) * pad], fix)
                out.append(y - fix)
            return tuple(out)

        values = lax.fori_loop(0, NMAX, step, tuple(starts), unroll=UNROLL)
        for cells, value in zip(groups, values):
            for i, (x, y) in enumerate(cells):
                ext2[x + 1, y + 1] = value[:, i * nz:(i + 1) * nz]

    y_arrive(0)

    def inner(c, carry):
        solve(tuple(range(1, nx - 1)), c * SPAN)
        return carry

    def outer(c, carry):
        per = SPAN // CHUNK
        for i in range(per):
            x_arrive(0, c * per + i)
        solve((0, nx - 1), c * SPAN)
        for side in (0, 1):
            @pl.when(has_x[side])
            def _():
                for i in range(per):
                    x_copy(1, side, c * per + i).start()
        return carry

    spans = ny // SPAN
    early = (spans + 1) // 2
    if nx > 2:
        lax.fori_loop(0, early, inner, 0)
    lax.fori_loop(0, spans, outer, 0)
    if nx > 2:
        lax.fori_loop(early, spans, inner, 0)
    for side in (0, 1):
        @pl.when(has_y[side])
        def _():
            y_copy(1, side).start()

    def finish(x, y):
        v, lap = laplace(ext2, x, y)
        new = v + 0.5 * (coef[...] * lap - forcing[x, y])
        out_ref[pl.ds(x * ny + y, spec, stride=rows), :] = new[:spec]

    for x in range(1, nx - 1):
        for y in range(1, ny - 1):
            finish(x, y)
    y_arrive(1)
    for x in range(1, nx - 1):
        finish(x, 0)
        finish(x, ny - 1)

    def last(c, carry):
        x_arrive(1, c)
        for j in range(CHUNK):
            for x in (0, nx - 1):
                finish(x, c * CHUNK + j)
        return carry

    lax.fori_loop(0, chunks, last, 0)

    for stage in (0, 1):
        for side in (0, 1):
            @pl.when(has_x[side])
            def _():
                for c in range(chunks):
                    x_copy(stage, side, c).wait_send()
            @pl.when(has_y[side])
            def _():
                y_copy(stage, side).wait_send()


def local(species, diffusion, class_rate, mixing, inverses, newton_counts, cell_class):
    spec, nx, ny, nz = species.shape
    nclass = inverses.shape[0]
    pad = -(-spec // 8) * 8
    chunks = ny // CHUNK
    width = 2 * GROUP * nz
    vmem = pl.BlockSpec(memory_space=pltpu.VMEM)
    smem = pl.BlockSpec(memory_space=pltpu.SMEM)
    out = pl.pallas_call(
        functools.partial(kernel, (spec, nx, ny, nz, nclass)),
        out_shape=pltpu.VMEM((spec * nx * ny, nz), F32),
        in_specs=[pl.BlockSpec(memory_space=pl.ANY), vmem, smem, vmem, vmem, smem, vmem],
        out_specs=vmem,
        scratch_shapes=[
            pltpu.VMEM((spec * nx * ny, nz), F32),
            pltpu.VMEM((nx + 2, ny + 2, pad, nz), F32),
            pltpu.VMEM((nx + 2, ny + 2, pad, nz), F32),
            pltpu.VMEM((nx, ny, pad, nz), F32),
            pltpu.VMEM((SPAN // GROUP, pad, width), F32),
            pltpu.VMEM((pad, nz), F32),
            pltpu.VMEM((64, 128), F32),
            pltpu.VMEM((64, 192), BF16),
            pltpu.VMEM((nclass * pad, 192), BF16),
            pltpu.SemaphoreType.DMA(()),
            pltpu.SemaphoreType.DMA((2, 2, chunks)),
            pltpu.SemaphoreType.DMA((2, 2, chunks)),
            pltpu.SemaphoreType.DMA((2, 2)),
            pltpu.SemaphoreType.DMA((2, 2)),
        ],
        compiler_params=pltpu.CompilerParams(
            collective_id=0, has_side_effects=True, vmem_limit_bytes=60 * 1024 * 1024),
    )(
        species.reshape(spec * nx * ny, nz), diffusion.reshape(1, spec), class_rate,
        mixing, inverses.transpose(1, 0, 2), newton_counts, cell_class.reshape(nx * ny, nz),
    )
    return out.reshape(species.shape)


def solution(mesh):
    in_specs = (P(None, "gx", "gy", None), P(), P(), P(), P(), P(), P("gx", "gy", None))
    out_specs = P(None, "gx", "gy", None)
    return jax.shard_map(local, mesh=mesh, in_specs=in_specs, out_specs=out_specs, check_vma=False)
```
